32 devices in a mesh: parts: 1 (over z), data: 32 (over y, x, core).
Axes of the slice: x: 4, y: 4, z: 1, core: 2. Of those that a mesh axis runs over, the one named last changes fastest.
The devices are a block of a 4x4x8 slice.
Arguments:
- feat_rows: bfloat16 [131072, 54], P('data')
- labels: int32 [131072], P('data')
- pos_init: float32 [54, 128], P(None, 'parts')
- mom_init: float32 [54, 128], P(None, 'parts')
- step_sizes: float32 [64, 128], P(None, 'parts')
Outputs:
- output 1: float32 [54, 128], P(None, 'parts')
- output 2: float32 [54, 128], P(None, 'parts')
- output 3: float32 [64, 128], P(None, 'parts')
All inputs are finite; a program needn't handle non-finite values.
Results may differ from the reference program's by a relative error of at most 0.001.
Values are sent between devices in bfloat16 or wider.
A program may use at most 768 MiB of HBM per device.

```python
import jax
import jax.numpy as jnp
from jax import lax

ROWS_DEV = 4096
GROUP_DEVS = 32
FEATURES = 54
CHAINS = 128
LEAPFROG = 64

ROWS_TOTAL = ROWS_DEV * GROUP_DEVS
PRIOR_VAR = 4.0
STEP_BASE = (ROWS_DEV + ROWS_TOTAL / FEATURES) ** -0.5
MOM_SCALE = (ROWS_TOTAL / FEATURES) ** 0.5


def setup_inputs(seed: int = 0, part: int = 0) -> dict:
    base_key = jax.random.key(seed)
    key_rate, key_label, key_noise, key_dir, key_strong = jax.random.split(base_key, 5)
    part_key = jax.random.fold_in(jax.random.key(seed + 1), part)
    key_pos, key_mom, key_step = jax.random.split(part_key, 3)
    shard_of_row = jnp.arange(ROWS_TOTAL) // ROWS_DEV
    label_rate = jax.random.randint(key_rate, (GROUP_DEVS,), 1, 16)
    label_draws = jax.random.randint(key_label, (ROWS_TOTAL,), 0, 16)
    labels = (label_draws < label_rate[shard_of_row]).astype(jnp.int32)
    label_sign = (2 * labels - 1).astype(jnp.float32)
    direction = jax.random.normal(key_dir, (FEATURES,), jnp.float32)
    noise_vals = jax.random.normal(key_noise, (ROWS_TOTAL, FEATURES), jnp.float32)
    noise_part = (0.5 / FEATURES ** 0.5) * (noise_vals + label_sign[:, None] * direction[None, :] / FEATURES ** 0.5)
    col_index = jnp.arange(FEATURES)
    strong_mask = ((col_index[None, :] % GROUP_DEVS) == (shard_of_row[:, None] % FEATURES)).astype(jnp.float32)
    strong_count = jnp.sum(strong_mask, axis=1, keepdims=True)
    strong_vals = 1.0 + 0.5 * jax.random.normal(key_strong, (ROWS_TOTAL, FEATURES), jnp.float32)
    feat_rows = (noise_part + strong_mask * strong_vals / jnp.sqrt(strong_count)).astype(jnp.bfloat16)
    pos_init = 0.5 * jax.random.normal(key_pos, (FEATURES, CHAINS), jnp.float32)
    mom_init = (0.5 * MOM_SCALE) * jax.random.normal(key_mom, (FEATURES, CHAINS), jnp.float32)
    step_sizes = STEP_BASE * jax.random.uniform(key_step, (LEAPFROG, CHAINS), jnp.float32, 0.6, 0.9)
    return {"feat_rows": feat_rows, "labels": labels, "pos_init": pos_init, "mom_init": mom_init, "step_sizes": step_sizes}


def potential_terms(feat_rows, labels, positions):
    pos_half = positions.astype(jnp.bfloat16)
    feat_blocks = feat_rows.reshape(GROUP_DEVS, ROWS_DEV, FEATURES)
    label_blocks = labels.astype(jnp.float32).reshape(GROUP_DEVS, ROWS_DEV, 1)

    def block_step(running, block_in):
        grad_acc, loss_acc = running
        block_rows, block_labels = block_in
        logits = jnp.dot(block_rows, pos_half, preferred_element_type=jnp.float32)
        residual = (block_labels - jax.nn.sigmoid(logits)).astype(jnp.bfloat16)
        grad_acc = grad_acc + jnp.dot(block_rows.T, residual, preferred_element_type=jnp.float32)
        loss_acc = loss_acc + jnp.sum(jax.nn.softplus(logits) - block_labels * logits, axis=0)
        return (grad_acc, loss_acc), None

    zero_state = (jnp.zeros((FEATURES, CHAINS), jnp.float32), jnp.zeros((CHAINS,), jnp.float32))
    (grad_lik, loss_lik), _ = lax.scan(block_step, zero_state, (feat_blocks, label_blocks))
    gradient = grad_lik - positions / PRIOR_VAR
    potential = loss_lik + jnp.sum(positions * positions, axis=0) / (2.0 * PRIOR_VAR)
    return gradient, potential


def reference(feat_rows, labels, pos_init, mom_init, step_sizes):
    grad_init, _ = potential_terms(feat_rows, labels, pos_init)

    def leap_step(loop_state, step_size):
        positions, momentum, gradient = loop_state
        momentum = momentum + 0.5 * step_size * gradient
        positions = positions + step_size * momentum
        gradient, potential = potential_terms(feat_rows, labels, positions)
        momentum = momentum + 0.5 * step_size * gradient
        energy = potential + 0.5 * jnp.sum(momentum * momentum, axis=0)
        return (positions, momentum, gradient), energy

    (positions, momentum, _), energies = lax.scan(leap_step, (pos_init, mom_init, grad_init), step_sizes)
    return positions, momentum, energies
```

```python
import functools

import jax
import jax.numpy as jnp
from jax import lax
from jax.experimental import pallas as pl
from jax.experimental.pallas import tpu as pltpu
from jax.sharding import PartitionSpec as P

PRIOR_VAR = 4.0
MESH = pl.DeviceIdType.MESH
SHARERS = 2
LANES = 128
FPAD = 64
BLOCKS = 4


def chain_kernel(
    n_dev, xt_ref, x_ref, pos_ref, mom_ref, step_ref, pos_out, mom_out, energy_out,
    eps_buf, part_buf, mine_buf, gath_buf, send_sem, recv_sem, fin_send, fin_recv, hsend, hrecv, hmine, hpart,
):
    feats, chains_all = pos_ref.shape
    steps = step_ref.shape[0]
    groups = n_dev // SHARERS
    chains = chains_all // groups
    n_chunk = xt_ref.shape[0]
    me = lax.axis_index("data")
    share = lax.rem(me, SHARERS)
    group = me // SHARERS
    lane = lax.broadcasted_iota(jnp.int32, (chains, LANES), 1)
    low = lane < FPAD

    barrier = pltpu.get_barrier_semaphore()
    for off in range(1, n_dev):
        pl.semaphore_signal(barrier, inc=1, device_id={"data": lax.rem(me + off, n_dev)}, device_id_type=MESH)
    pl.semaphore_wait(barrier, n_dev - 1)

    def own_rows(ref):
        rows = ref.shape[0]
        padded = jnp.concatenate([ref[...], jnp.zeros((LANES - rows, chains_all), jnp.float32)], axis=0)
        return padded.T

    def doubled(ref, buf):
        wide = own_rows(ref)
        wide = jnp.where(lax.broadcasted_iota(jnp.int32, wide.shape, 1) < FPAD, wide, 0.0)
        buf[...] = wide + pltpu.roll(wide, FPAD, 1)
        return buf[pl.ds(pl.multiple_of(group * chains, chains), chains), :]

    theta0 = doubled(pos_ref, gath_buf.at[0])
    mom0 = doubled(mom_ref, gath_buf.at[0])
    eps_rows = doubled(step_ref, gath_buf.at[0])
    for l in range(steps):
        eps_buf[l + 1] = jnp.broadcast_to(eps_rows[:, l : l + 1], (chains, LANES))
    eps_buf[0] = jnp.zeros((chains, LANES), jnp.float32)

    def step_body(l, state):
        theta, mom, grad, carried, hmat = state
        eps = eps_buf[l]
        start_mom = mom
        mom = mom + 0.5 * eps * grad
        theta = theta + eps * mom

        half = 0.5 * theta
        left, right, none = jnp.where(low, half, 0.0), jnp.where(low, 0.0, half), jnp.zeros_like(half)
        weights = jnp.concatenate(
            [
                jnp.concatenate([left, none], axis=1),
                jnp.concatenate([right, none], axis=1),
                jnp.concatenate([none, left], axis=1),
                jnp.concatenate([none, right], axis=1),
            ],
            axis=0,
        ).astype(jnp.bfloat16)

        total = jnp.zeros((BLOCKS * chains, BLOCKS * FPAD), jnp.float32)
        ramp = jnp.zeros((BLOCKS * chains, 256), jnp.float32)
        prod = jnp.ones((BLOCKS * chains, 256), jnp.float32)
        for k in range(n_chunk):
            u = jnp.dot(weights, xt_ref[k], preferred_element_type=jnp.float32)
            h = jnp.tanh(u)
            resid = (1.0 + h).astype(jnp.bfloat16)
            total = total + jnp.dot(resid, x_ref[k], preferred_element_type=jnp.float32)
            pos_part = jnp.maximum(u, 0.0)
            fac = 1.0 + jnp.abs(h)
            for q in range(u.shape[1] // 256):
                ramp = ramp + pos_part[:, q * 256 : (q + 1) * 256]
                prod = prod * fac[:, q * 256 : (q + 1) * 256]

        blocks = [total[b * chains : (b + 1) * chains] for b in range(BLOCKS)]
        diag = jnp.where(low, blocks[0][:, :LANES] + blocks[2][:, LANES:], blocks[1][:, :LANES] + blocks[3][:, LANES:])
        mine = diag + pltpu.roll(diag, FPAD, 1)
        slot = lax.rem(l, 2)
        mine_buf[slot] = mine
        part_buf[slot, share] = mine
        copies = []
        for off in range(1, SHARERS):
            peer = group * SHARERS + lax.rem(share + off, SHARERS)
            copies.append(
                pltpu.make_async_remote_copy(
                    src_ref=mine_buf.at[slot],
                    dst_ref=part_buf.at[slot, share],
                    send_sem=send_sem.at[slot, off - 1],
                    recv_sem=recv_sem.at[slot, off - 1],
                    device_id={"data": peer},
                    device_id_type=MESH,
                )
            )
        for copy in copies:
            copy.start()

        kinetic = jnp.where(low, start_mom * start_mom * (0.5 / SHARERS), 0.0)
        hmat = jnp.where(lane == l - 2, jnp.sum(carried + kinetic, axis=1, keepdims=True), hmat)
        factors = SHARERS * 4096
        loss = 2.0 * ramp - jnp.log(prod)
        loss = loss[:, :LANES] + loss[:, LANES:]
        loss = loss[:chains] + loss[chains : 2 * chains] + loss[2 * chains : 3 * chains] + loss[3 * chains :]
        rows_per_lane = n_chunk * xt_ref.shape[2] * BLOCKS // LANES
        loss = loss + rows_per_lane * 0.6931471805599453
        carried = loss + jnp.where(low, theta * theta * (0.5 / PRIOR_VAR / SHARERS), 0.0)

        for copy in copies:
            copy.wait()
        summed = part_buf[slot, 0]
        for s in range(1, SHARERS):
            summed = summed + part_buf[slot, s]
        grad = -0.5 * summed - theta / PRIOR_VAR
        mom = mom + 0.5 * eps * grad
        return theta, mom, grad, carried, hmat

    zero = jnp.zeros((chains, LANES), jnp.float32)
    theta, mom, _, carried, hmat = lax.fori_loop(0, steps + 1, step_body, (theta0, mom0, zero, zero, zero))
    kinetic = jnp.where(low, mom * mom * (0.5 / SHARERS), 0.0)
    hmat = jnp.where(lane == steps - 1, jnp.sum(carried + kinetic, axis=1, keepdims=True), hmat)

    hmine[...] = hmat
    hpart[share] = hmat
    copies = []
    for off in range(1, SHARERS):
        peer = group * SHARERS + lax.rem(share + off, SHARERS)
        copies.append(
            pltpu.make_async_remote_copy(
                src_ref=hmine,
                dst_ref=hpart.at[share],
                send_sem=hsend.at[off - 1],
                recv_sem=hrecv.at[off - 1],
                device_id={"data": peer},
                device_id_type=MESH,
            )
        )
    for copy in copies:
        copy.start()
    for copy in copies:
        copy.wait()
    hsum = hpart[0]
    for s in range(1, SHARERS):
        hsum = hsum + hpart[s]

    rows = pl.ds(pl.multiple_of(group * chains, chains), chains)
    gath_buf[1, rows, :] = jnp.where(low, theta, mom)
    gath_buf[2, rows, :] = hsum
    copies = []
    for off in range(1, groups):
        peer = lax.rem(group + off, groups) * SHARERS + share
        copies.append(
            pltpu.make_async_remote_copy(
                src_ref=gath_buf.at[pl.ds(1, 2), rows, :],
                dst_ref=gath_buf.at[pl.ds(1, 2), rows, :],
                send_sem=fin_send.at[off - 1],
                recv_sem=fin_recv.at[off - 1],
                device_id={"data": peer},
                device_id_type=MESH,
            )
        )
    for copy in copies:
        copy.start()
    for copy in copies:
        copy.wait()
    both = gath_buf[1].T
    pos_out[...] = both[:feats]
    mom_out[...] = both[FPAD : FPAD + feats]
    energy_out[...] = gath_buf[2].T[:steps]


def solution(mesh):
    n_dev = mesh.shape["data"]
    groups = n_dev // SHARERS
    row_spec = P("data", None)
    chain_spec = P(None, "parts")

    def local_chains(feat_rows, labels, pos_init, mom_init, step_sizes):
        rows, feats = feat_rows.shape
        chains_all = pos_init.shape[1]
        steps = step_sizes.shape[0]
        chains = chains_all // groups
        signed = feat_rows * (1 - 2 * labels).astype(jnp.bfloat16)[:, None]
        signed = jnp.pad(signed, ((0, 0), (0, FPAD - feats)))
        packed = signed.reshape(BLOCKS, rows // BLOCKS, FPAD).transpose(1, 0, 2).reshape(rows // BLOCKS, BLOCKS * FPAD)
        same_share = [[g * SHARERS + s for g in range(groups)] for s in range(SHARERS)]
        x_all = lax.all_gather(packed, "data", axis_index_groups=same_share)
        xt_all = x_all.transpose(0, 2, 1)

        vmem = pl.BlockSpec(memory_space=pltpu.VMEM)
        dma = pltpu.SemaphoreType.DMA
        return pl.pallas_call(
            functools.partial(chain_kernel, n_dev),
            out_shape=(
                jax.ShapeDtypeStruct(pos_init.shape, jnp.float32),
                jax.ShapeDtypeStruct(mom_init.shape, jnp.float32),
                jax.ShapeDtypeStruct(step_sizes.shape, jnp.float32),
            ),
            in_specs=[vmem] * 5,
            out_specs=(vmem, vmem, vmem),
            scratch_shapes=[
                pltpu.VMEM((steps + 1, chains, LANES), jnp.float32),
                pltpu.VMEM((2, SHARERS, chains, LANES), jnp.float32),
                pltpu.VMEM((2, chains, LANES), jnp.float32),
                pltpu.VMEM((3, chains_all, LANES), jnp.float32),
                dma((2, SHARERS - 1)),
                dma((2, SHARERS - 1)),
                dma((groups - 1,)),
                dma((groups - 1,)),
                dma((SHARERS - 1,)),
                dma((SHARERS - 1,)),
                pltpu.VMEM((chains, LANES), jnp.float32),
                pltpu.VMEM((SHARERS, chains, LANES), jnp.float32),
            ],
            compiler_params=pltpu.CompilerParams(
                collective_id=0, has_side_effects=True, vmem_limit_bytes=60 * 1024 * 1024
            ),
        )(xt_all, x_all, pos_init, mom_init, step_sizes)

    return jax.shard_map(local_chains, mesh=mesh, in_specs=(row_spec, P("data"), chain_spec, chain_spec, chain_spec), out_specs=(chain_spec, chain_spec, chain_spec), check_vma=False)
```

```python
import functools
import math

import jax
import jax.numpy as jnp
from jax import lax
from jax.experimental import pallas as pl
from jax.experimental.pallas import tpu as pltpu
from jax.sharding import PartitionSpec as P

PRIOR_VAR = 4.0
MESH = pl.DeviceIdType.MESH
CORES = 2
LANES = 128
FPAD = 64
BLOCKS = 4
TILE = 256
MID_LAG, GRAD_LAG, SWAP_LAG = 3, 4, 4
LN2 = 0.6931471805599453
OFFSETS = [(dx, dy) for dy in (0, -1, 1, 2) for dx in (0, -1, 1, 2)]
SHARED = [(0, 0), (-1, 0), (1, 0)]
ALONE = [o for o in OFFSETS if o not in SHARED]


def chain_kernel(
    n_dev, own_ref, pos_ref, mom_ref, step_ref, pos_out, mom_out, energy_out,
    xs, xt, eps_buf, part_buf, mine_buf, gath_buf,
    send_sem, recv_sem, fin_send, fin_recv, g_send, g_recv, d_send, d_recv, own_sem,
):
    feats, chains_all = pos_ref.shape
    steps = step_ref.shape[0]
    n_chip = n_dev // CORES
    side = math.isqrt(n_chip)
    chains = chains_all // n_chip
    pack_rows = own_ref.shape[0]
    half_rows, quarter = pack_rows // 2, pack_rows // 4
    n_slots = len(ALONE) + CORES * len(SHARED)
    me = lax.axis_index("data")
    core = lax.rem(me, CORES)
    chip = me // CORES
    chip_x, chip_y = lax.rem(chip, side), chip // side
    lane = lax.broadcasted_iota(jnp.int32, (chains, LANES), 1)
    low = lane < FPAD
    partner = {"data": chip * CORES + 1 - core}

    def neighbour(axis, step):
        nx = lax.rem(chip_x + side + step, side) if axis == 0 else chip_x
        ny = lax.rem(chip_y + side + step, side) if axis == 1 else chip_y
        return {"data": (ny * side + nx) * CORES + core}

    barrier = pltpu.get_barrier_semaphore()
    for off in range(1, n_dev):
        pl.semaphore_signal(barrier, inc=1, device_id={"data": lax.rem(me + off, n_dev)}, device_id_type=MESH)
    pl.semaphore_wait(barrier, n_dev - 1)

    def slot_of(offset):
        if offset in SHARED:
            return len(ALONE) + SHARED.index(offset) * CORES + core
        return ALONE.index(offset)

    sends = []

    def send(src, dst_slot, rows, sem, axis, step):
        copy = pltpu.make_async_remote_copy(
            src_ref=src,
            dst_ref=xs.at[dst_slot, rows, :],
            send_sem=g_send.at[len(sends)],
            recv_sem=g_recv.at[sem],
            device_id=neighbour(axis, step),
            device_id_type=MESH,
        )
        copy.start()
        sends.append(copy)

    def offset_of(half, first, second):
        return (first, second) if half == 0 else (second, first)

    def rows_of(half, part):
        if part is None:
            return pl.ds(half * half_rows, half_rows)
        return pl.ds(half * half_rows + part * quarter, quarter)

    kinds = [(1, None), (-1, None), (2, 0), (2, 1)]
    sem_ids = {}
    for half in range(2):
        for kind in kinds:
            sem_ids[half, kind[0], 0, kind[1]] = len(sem_ids)
            for first in (0, -1, 1, 2):
                sem_ids[half, first, kind[0], kind[1]] = len(sem_ids)

    def piece(half, first, second, part):
        return xs.at[slot_of(offset_of(half, first, second)), rows_of(half, part), :]

    def wrap(v):
        return 2 if v == -2 else v

    def pass_on(half, first, second, part, along, step, to_part=None):
        axis = along if half == 0 else 1 - along
        src_part = part if to_part is None else to_part
        if (first, second) == (0, 0):
            src = own_ref.at[rows_of(half, src_part), :]
        else:
            src = piece(half, first, second, src_part)
        nf, ns = (wrap(first - step), second) if along == 0 else (first, wrap(second - step))
        key = (half, nf, ns, to_part)
        send(src, slot_of(offset_of(half, nf, ns)), rows_of(half, src_part), sem_ids[key], axis, step)

    def arrive(half, first, second, part):
        dst = piece(half, first, second, part)
        pltpu.make_async_copy(dst, dst, g_recv.at[sem_ids[half, first, second, part]]).wait()

    handed = []

    def hand_over(half, offset, src):
        index = SHARED.index(offset) * 2 + half
        copy = pltpu.make_async_remote_copy(
            src_ref=src,
            dst_ref=xs.at[slot_of(offset), rows_of(half, None), :],
            send_sem=d_send.at[index],
            recv_sem=d_recv.at[index],
            device_id=partner,
            device_id_type=MESH,
        )
        copy.start()
        handed.append(copy)

    def turn(slot, half):
        def turn_part(i, _):
            rows = pl.ds(pl.multiple_of(half * half_rows + i * quarter, quarter), quarter)
            xt[slot, :, rows] = xs[slot, rows, :].T
            return 0

        lax.fori_loop(0, 2, turn_part, 0)

    for half in range(2):
        for step in (1, -1):
            pass_on(half, 0, 0, None, 0, step)
    for half in range(2):
        for step in (1, -1):
            pass_on(half, 0, 0, None, 1, step)
    own_slot = slot_of((0, 0))
    own_copy = pltpu.make_async_copy(own_ref, xs.at[own_slot], own_sem.at[0])
    own_copy.start()
    for half in range(2):
        hand_over(half, (0, 0), own_ref.at[rows_of(half, None), :])

    def own_rows(ref):
        rows = ref.shape[0]
        padded = jnp.concatenate([ref[...], jnp.zeros((LANES - rows, chains_all), jnp.float32)], axis=0)
        return padded.T

    def doubled(ref, buf):
        wide = own_rows(ref)
        buf[...] = wide + pltpu.roll(wide, FPAD, 1)
        return buf[pl.ds(pl.multiple_of(chip * chains, chains), chains), :]

    theta0 = doubled(pos_ref, gath_buf.at[0])
    mom0 = doubled(mom_ref, gath_buf.at[0])
    eps_rows = doubled(step_ref, gath_buf.at[0])
    for l in range(steps):
        eps_buf[l + 1] = jnp.broadcast_to(eps_rows[:, l : l + 1], (chains, LANES))
    eps_buf[0] = jnp.zeros((chains, LANES), jnp.float32)
    own_copy.wait()
    for half in range(2):
        turn(own_slot, half)

    def landed(half, first, second):
        offset = offset_of(half, first, second)
        if offset in SHARED:
            hand_over(half, offset, piece(half, first, second, None))

    fresh = []
    for half in range(2):
        for first in (-1, 1):
            arrive(half, first, 0, None)
            pass_on(half, first, 0, None, 0, -first, to_part=0 if first < 0 else 1)
            for step in (1, -1):
                pass_on(half, first, 0, None, 1, step)
            landed(half, first, 0)
            fresh.append((half, first, 0))

    def turn_fresh():
        for half, first, second in fresh:
            turn(slot_of(offset_of(half, first, second)), half)
        fresh.clear()

    turn_fresh()

    def second_ring(first):
        for half in range(2):
            for second in (-1, 1):
                arrive(half, first, second, None)
                pass_on(half, first, second, None, 1, -second, to_part=0 if second < 0 else 1)
                landed(half, first, second)
                fresh.append((half, first, second))

    second_ring(0)
    for half in range(2):
        for part in range(2):
            arrive(half, 2, 0, part)
        for step in (1, -1):
            pass_on(half, 2, 0, None, 1, step)
        fresh.append((half, 2, 0))
    turn_fresh()
    second_ring(-1)
    second_ring(1)
    turn_fresh()
    second_ring(2)
    for copy in handed:
        copy.wait_recv()
    for i, offset in enumerate(SHARED):
        for half in range(2):
            turn(len(ALONE) + i * CORES + 1 - core, half)
    for first in (0, -1, 1):
        for half in range(2):
            for part in range(2):
                arrive(half, first, 2, part)
            fresh.append((half, first, 2))
    turn_fresh()
    for half in range(2):
        for part in range(2):
            arrive(half, 2, 2, part)
        fresh.append((half, 2, 2))
    turn_fresh()
    for copy in sends:
        copy.wait_send()
    for copy in handed:
        copy.wait_send()

    def step_body(l, state):
        theta, mom, grad, carried, hmat = state
        eps = eps_buf[l]
        start_mom = mom
        mom = mom + 0.5 * eps * grad
        theta = theta + eps * mom

        half = 0.5 * theta
        left, right, none = jnp.where(low, half, 0.0), jnp.where(low, 0.0, half), jnp.zeros_like(half)
        weights = jnp.concatenate(
            [
                jnp.concatenate([left, none], axis=1),
                jnp.concatenate([right, none], axis=1),
                jnp.concatenate([none, left], axis=1),
                jnp.concatenate([none, right], axis=1),
            ],
            axis=0,
        ).astype(jnp.bfloat16)

        def gather_blocks(total):
            blocks = [total[b * chains : (b + 1) * chains] for b in range(BLOCKS)]
            diag = jnp.where(low, blocks[0][:, :LANES] + blocks[2][:, LANES:], blocks[1][:, :LANES] + blocks[3][:, LANES:])
            return diag + pltpu.roll(diag, FPAD, 1)

        def fold(sums):
            loss = 2.0 * sums[0] - jnp.log(sums[1])
            return loss[:chains] + loss[chains : 2 * chains] + loss[2 * chains : 3 * chains] + loss[3 * chains :]

        no_sums = (jnp.zeros((BLOCKS * chains, LANES), jnp.float32), jnp.ones((BLOCKS * chains, LANES), jnp.float32))
        slot = lax.rem(l, 2)
        copy = pltpu.make_async_remote_copy(
            src_ref=mine_buf.at[slot],
            dst_ref=part_buf.at[slot],
            send_sem=send_sem.at[slot],
            recv_sem=recv_sem.at[slot],
            device_id=partner,
            device_id_type=MESH,
        )
        per_shard = pack_rows // TILE
        tiles = [(k, slice(c * TILE, (c + 1) * TILE)) for k in range(n_slots) for c in range(per_shard)]
        n_alone = len(ALONE) * per_shard
        sums = [no_sums, no_sums]
        totals = [jnp.zeros((BLOCKS * chains, BLOCKS * FPAD), jnp.float32)] * 2
        logits, resids = {}, {}
        mine = None
        for turn_no in range(len(tiles) + GRAD_LAG):
            if turn_no < len(tiles):
                k, cols = tiles[turn_no]
                logits[turn_no] = jnp.dot(weights, xt[k, :, cols], preferred_element_type=jnp.float32)
            tile = turn_no - MID_LAG
            if 0 <= tile < len(tiles):
                u = logits.pop(tile)
                h = jnp.tanh(u)
                pos_part = jnp.maximum(u, 0.0)
                fac = 1.0 + jnp.abs(h)
                ramp, prod = sums[tile >= n_alone]
                for q in range(TILE // 256):
                    lo, hi = slice(q * 256, q * 256 + LANES), slice(q * 256 + LANES, (q + 1) * 256)
                    ramp = ramp + (pos_part[:, lo] + pos_part[:, hi])
                    prod = prod * (fac[:, lo] * fac[:, hi])
                sums[tile >= n_alone] = (ramp, prod)
                resids[tile] = (1.0 + h).astype(jnp.bfloat16)
            tile = turn_no - GRAD_LAG
            if tile >= 0:
                k, rows = tiles[tile]
                part = jnp.dot(resids.pop(tile), xs[k, rows, :], preferred_element_type=jnp.float32)
                totals[tile >= n_alone] = totals[tile >= n_alone] + part
            if tile == n_alone - 1 + SWAP_LAG:
                mine = gather_blocks(totals[0])
                mine_buf[slot] = mine
                copy.start()
        both = gather_blocks(totals[1])
        sums_alone, sums_both = sums

        kinetic = jnp.where(low, start_mom * start_mom * (0.5 / CORES), 0.0)
        hmat = jnp.where(lane == l - 2, jnp.sum(carried + kinetic, axis=1, keepdims=True), hmat)
        loss = fold(sums_alone) + (1.0 / CORES) * fold(sums_both)
        loss = loss + (n_chip * pack_rows * BLOCKS // LANES) * LN2
        carried = loss + jnp.where(low, theta * theta * (0.5 / PRIOR_VAR / CORES), 0.0)

        copy.wait()
        grad = -0.5 * ((mine + part_buf[slot]) + both) - theta / PRIOR_VAR
        mom = mom + 0.5 * eps * grad
        return theta, mom, grad, carried, hmat

    zero = jnp.zeros((chains, LANES), jnp.float32)
    theta, mom, _, carried, hmat = lax.fori_loop(0, steps + 1, step_body, (theta0, mom0, zero, zero, zero))
    kinetic = jnp.where(low, mom * mom * (0.5 / CORES), 0.0)
    hmat = jnp.where(lane == steps - 1, jnp.sum(carried + kinetic, axis=1, keepdims=True), hmat)

    last = (steps + 1) % 2
    mine_buf[last] = hmat
    copy = pltpu.make_async_remote_copy(
        src_ref=mine_buf.at[last],
        dst_ref=part_buf.at[last],
        send_sem=send_sem.at[last],
        recv_sem=recv_sem.at[last],
        device_id=partner,
        device_id_type=MESH,
    )
    copy.start()
    copy.wait()

    rows = pl.ds(pl.multiple_of(chip * chains, chains), chains)
    gath_buf[1, rows, :] = jnp.where(low, theta, mom)
    gath_buf[2, rows, :] = hmat + part_buf[last]
    copies = []
    for off in range(1, n_chip):
        copies.append(
            pltpu.make_async_remote_copy(
                src_ref=gath_buf.at[pl.ds(1, 2), rows, :],
                dst_ref=gath_buf.at[pl.ds(1, 2), rows, :],
                send_sem=fin_send.at[off - 1],
                recv_sem=fin_recv.at[off - 1],
                device_id={"data": lax.rem(chip + off, n_chip) * CORES + core},
                device_id_type=MESH,
            )
        )
    for copy in copies:
        copy.start()
    for copy in copies:
        copy.wait()
    ends = gath_buf[1].T
    pos_out[...] = ends[:feats]
    mom_out[...] = ends[FPAD : FPAD + feats]
    energy_out[...] = gath_buf[2].T[:steps]


def solution(mesh):
    n_dev = mesh.shape["data"]
    n_chip = n_dev // CORES
    row_spec = P("data", None)
    chain_spec = P(None, "parts")

    def local_chains(feat_rows, labels, pos_init, mom_init, step_sizes):
        rows, feats = feat_rows.shape
        chains_all = pos_init.shape[1]
        steps = step_sizes.shape[0]
        chains = chains_all // n_chip
        pack_rows, pack_cols = rows // BLOCKS, BLOCKS * FPAD
        signed = feat_rows * (1 - 2 * labels).astype(jnp.bfloat16)[:, None]
        signed = jnp.pad(signed, ((0, 0), (0, FPAD - feats)))
        packed = signed.reshape(BLOCKS, pack_rows, FPAD).transpose(1, 0, 2).reshape(pack_rows, pack_cols)

        vmem = pl.BlockSpec(memory_space=pltpu.VMEM)
        dma = pltpu.SemaphoreType.DMA
        slots = len(ALONE) + CORES * len(SHARED)
        return pl.pallas_call(
            functools.partial(chain_kernel, n_dev),
            out_shape=(
                jax.ShapeDtypeStruct(pos_init.shape, jnp.float32),
                jax.ShapeDtypeStruct(mom_init.shape, jnp.float32),
                jax.ShapeDtypeStruct(step_sizes.shape, jnp.float32),
            ),
            in_specs=[vmem] * 4,
            out_specs=(vmem, vmem, vmem),
            scratch_shapes=[
                pltpu.VMEM((slots, pack_rows, pack_cols), jnp.bfloat16),
                pltpu.VMEM((slots, pack_cols, pack_rows), jnp.bfloat16),
                pltpu.VMEM((steps + 1, chains, LANES), jnp.float32),
                pltpu.VMEM((2, chains, LANES), jnp.float32),
                pltpu.VMEM((2, chains, LANES), jnp.float32),
                pltpu.VMEM((3, chains_all, LANES), jnp.float32),
                dma((2,)),
                dma((2,)),
                dma((n_chip - 1,)),
                dma((n_chip - 1,)),
                dma((40,)),
                dma((40,)),
                dma((2 * len(SHARED),)),
                dma((2 * len(SHARED),)),
                dma((1,)),
            ],
            compiler_params=pltpu.CompilerParams(
                collective_id=0, has_side_effects=True, vmem_limit_bytes=60 * 1024 * 1024
            ),
        )(packed, pos_init, mom_init, step_sizes)

    return jax.shard_map(local_chains, mesh=mesh, in_specs=(row_spec, P("data"), chain_spec, chain_spec, chain_spec), out_specs=(chain_spec, chain_spec, chain_spec), check_vma=False)
```

```python
import functools
import math

import jax
import jax.numpy as jnp
from jax import lax
from jax.experimental import pallas as pl
from jax.experimental.pallas import tpu as pltpu
from jax.sharding import PartitionSpec as P

PRIOR_VAR = 4.0
MESH = pl.DeviceIdType.MESH
CORES = 2
LANES = 128
FPAD = 56
BLOCKS = 16
UNIT = 8
MID_LAG, GRAD_LAG, SWAP_LAG = 2, 3, 2
LN2 = 0.6931471805599453
OFFSETS = [(dx, dy) for dy in (0, -1, 1, 2) for dx in (0, -1, 1, 2)]
SHARED = [(0, 0), (-1, 0), (1, 0)]
ALONE = [o for o in OFFSETS if o not in SHARED]


def chain_kernel(
    n_dev, rows_ref, label_ref, pos_ref, mom_ref, step_ref, all_out,
    xs, xt, eps_buf, part_buf, mine_buf, gath_buf,
    send_sem, recv_sem, fin_send, fin_recv, g_send, g_recv, d_send, d_recv,
):
    feats, chains_all = pos_ref.shape
    steps = step_ref.shape[0]
    n_chip = n_dev // CORES
    side = math.isqrt(n_chip)
    chains = chains_all // n_chip
    block_rows = xs.shape[1]
    width = BLOCKS * FPAD
    half_rows, quarter = width // 2, width // 4
    n_slots = len(ALONE) + CORES * len(SHARED)
    me = lax.axis_index("data")
    core = lax.rem(me, CORES)
    chip = me // CORES
    chip_x, chip_y = lax.rem(chip, side), chip // side
    lane = lax.broadcasted_iota(jnp.int32, (chains, LANES), 1)
    low = lane < feats
    partner = {"data": chip * CORES + 1 - core}

    def neighbour(axis, step):
        nx = lax.rem(chip_x + side + step, side) if axis == 0 else chip_x
        ny = lax.rem(chip_y + side + step, side) if axis == 1 else chip_y
        return {"data": (ny * side + nx) * CORES + core}

    barrier = pltpu.get_barrier_semaphore()
    for off in range(1, n_dev):
        pl.semaphore_signal(barrier, inc=1, device_id={"data": lax.rem(me + off, n_dev)}, device_id_type=MESH)

    def slot_of(offset):
        if offset in SHARED:
            return len(ALONE) + SHARED.index(offset) * CORES + core
        return ALONE.index(offset)

    sends = []

    def send(src, dst_slot, rows, sem, axis, step):
        copy = pltpu.make_async_remote_copy(
            src_ref=src,
            dst_ref=xt.at[dst_slot, rows, :],
            send_sem=g_send.at[len(sends)],
            recv_sem=g_recv.at[sem],
            device_id=neighbour(axis, step),
            device_id_type=MESH,
        )
        copy.start()
        sends.append(copy)

    def offset_of(half, first, second):
        return (first, second) if half == 0 else (second, first)

    def rows_of(half, part):
        if part is None:
            return pl.ds(half * half_rows, half_rows)
        return pl.ds(half * half_rows + part * quarter, quarter)

    kinds = [(1, None), (-1, None), (2, 0), (2, 1)]
    sem_ids = {}
    for half in range(2):
        for kind in kinds:
            sem_ids[half, kind[0], 0, kind[1]] = len(sem_ids)
            for first in (0, -1, 1, 2):
                sem_ids[half, first, kind[0], kind[1]] = len(sem_ids)

    def piece(half, first, second, part):
        return xt.at[slot_of(offset_of(half, first, second)), rows_of(half, part), :]

    def wrap(v):
        return 2 if v == -2 else v

    def pass_on(half, first, second, part, along, step, to_part=None):
        axis = along if half == 0 else 1 - along
        src_part = part if to_part is None else to_part
        src = piece(half, first, second, src_part)
        nf, ns = (wrap(first - step), second) if along == 0 else (first, wrap(second - step))
        key = (half, nf, ns, to_part)
        send(src, slot_of(offset_of(half, nf, ns)), rows_of(half, src_part), sem_ids[key], axis, step)

    def arrive(half, first, second, part):
        dst = piece(half, first, second, part)
        pltpu.make_async_copy(dst, dst, g_recv.at[sem_ids[half, first, second, part]]).wait()

    handed = []

    def hand_over(half, offset, src):
        index = SHARED.index(offset) * 2 + half
        copy = pltpu.make_async_remote_copy(
            src_ref=src,
            dst_ref=xt.at[slot_of(offset), rows_of(half, None), :],
            send_sem=d_send.at[index],
            recv_sem=d_recv.at[index],
            device_id=partner,
            device_id_type=MESH,
        )
        copy.start()
        handed.append(copy)

    seen = set()

    def turn(offset, half, slot):
        seen.add((offset, half))
        if (offset, 1 - half) not in seen:
            return

        def turn_part(i, _):
            rows = pl.ds(pl.multiple_of(i * LANES, LANES), LANES)
            xs[slot, :, rows] = xt[slot, rows, :].T
            return 0

        lax.fori_loop(0, width // LANES, turn_part, 0)

    own_slot = slot_of((0, 0))
    signs = (1 - 2 * label_ref[...]).astype(jnp.float32).astype(jnp.bfloat16)
    per_block = block_rows // LANES
    for j in range(BLOCKS * per_block):
        tile = rows_ref[:, j * LANES : (j + 1) * LANES] * signs[j : j + 1, :]
        tile = jnp.concatenate([tile, jnp.zeros((FPAD - feats, LANES), jnp.bfloat16)], axis=0)
        b, m = j // per_block, j % per_block
        xt[own_slot, b * FPAD : (b + 1) * FPAD, m * LANES : (m + 1) * LANES] = tile

    pl.semaphore_wait(barrier, n_dev - 1)
    for half in range(2):
        for step in (1, -1):
            pass_on(half, 0, 0, None, 0, step)
    for half in range(2):
        for step in (1, -1):
            pass_on(half, 0, 0, None, 1, step)
    for half in range(2):
        hand_over(half, (0, 0), piece(half, 0, 0, None))

    def own_rows(ref):
        rows = ref.shape[0]
        padded = jnp.concatenate([ref[...], jnp.zeros((LANES - rows, chains_all), jnp.float32)], axis=0)
        return padded.T

    def mine_of(ref, buf):
        buf[...] = own_rows(ref)
        return buf[pl.ds(pl.multiple_of(chip * chains, chains), chains), :]

    theta0 = mine_of(pos_ref, gath_buf.at[0])
    mom0 = mine_of(mom_ref, gath_buf.at[0])
    eps_rows = mine_of(step_ref, gath_buf.at[0])
    for l in range(steps):
        eps_buf[l + 1] = jnp.broadcast_to(eps_rows[:, l : l + 1], (chains, LANES))
    eps_buf[0] = jnp.zeros((chains, LANES), jnp.float32)
    for half in range(2):
        turn((0, 0), half, own_slot)

    def landed(half, first, second):
        offset = offset_of(half, first, second)
        if offset in SHARED:
            hand_over(half, offset, piece(half, first, second, None))

    fresh = []
    for half in range(2):
        for first in (-1, 1):
            arrive(half, first, 0, None)
            pass_on(half, first, 0, None, 0, -first, to_part=0 if first < 0 else 1)
            for step in (1, -1):
                pass_on(half, first, 0, None, 1, step)
            landed(half, first, 0)
            fresh.append((half, first, 0))

    def turn_fresh():
        for half, first, second in fresh:
            offset = offset_of(half, first, second)
            turn(offset, half, slot_of(offset))
        fresh.clear()

    turn_fresh()

    def second_ring(first):
        for half in range(2):
            for second in (-1, 1):
                arrive(half, first, second, None)
                pass_on(half, first, second, None, 1, -second, to_part=0 if second < 0 else 1)
                landed(half, first, second)
                fresh.append((half, first, second))

    second_ring(0)
    for half in range(2):
        for part in range(2):
            arrive(half, 2, 0, part)
        for step in (1, -1):
            pass_on(half, 2, 0, None, 1, step)
        fresh.append((half, 2, 0))
    turn_fresh()
    second_ring(-1)
    second_ring(1)
    turn_fresh()
    second_ring(2)
    for copy in handed:
        copy.wait_recv()
    for i, offset in enumerate(SHARED):
        for half in range(2):
            turn((offset, "partner"), half, len(ALONE) + i * CORES + 1 - core)
    for first in (0, -1, 1):
        for half in range(2):
            for part in range(2):
                arrive(half, first, 2, part)
            fresh.append((half, first, 2))
    turn_fresh()
    for half in range(2):
        for part in range(2):
            arrive(half, 2, 2, part)
        fresh.append((half, 2, 2))
    turn_fresh()
    for copy in sends:
        copy.wait_send()
    for copy in handed:
        copy.wait_send()

    def step_body(l, state):
        theta, mom, grad, carried, hmat = state
        eps = eps_buf[l]
        start_mom = mom
        mom = mom + 0.5 * eps * grad
        theta = theta + eps * mom

        half = 0.5 * theta
        none = jnp.zeros_like(half)
        rows_w = []
        for b in range(UNIT):
            col, start = b * FPAD // LANES, b * FPAD % LANES
            moved = pltpu.roll(half, start, 1) if start else half
            cols = [none] * (-(-UNIT * FPAD // LANES))
            if start + FPAD <= LANES:
                cols[col] = moved
            else:
                cols[col] = jnp.where(lane >= start, moved, 0.0)
                cols[col + 1] = jnp.where(lane >= start, 0.0, moved)
            rows_w.append(jnp.concatenate(cols, axis=1))
        weights = jnp.concatenate(rows_w, axis=0).astype(jnp.bfloat16)[:, : UNIT * FPAD]

        first_block = (0, 4, 8, 12)

        def gather_blocks(strips):
            result = None
            for b in range(BLOCKS):
                col, start = b * FPAD // LANES, b * FPAD % LANES

                def at(c):
                    strip = c // 2
                    row = (b - first_block[strip]) * chains
                    if strip < 3:
                        return strips[strip][row : row + chains, (c % 2) * LANES : (c % 2 + 1) * LANES]
                    other = row + 4 * chains
                    return strips[3][row : row + chains, :LANES] + strips[3][other : other + chains, LANES:]

                part = at(col)
                if start + feats > LANES:
                    part = jnp.where(lane >= start, part, at(col + 1))
                part = pltpu.roll(part, LANES - start, 1) if start else part
                result = part if result is None else result + part
            return jnp.where(low, result, 0.0)

        def fold(sums):
            loss = 2.0 * sums[0] - jnp.log(sums[1])
            return loss[:chains] + loss[chains : 2 * chains] + loss[2 * chains : 3 * chains] + loss[3 * chains :]

        no_sums = (jnp.zeros((4 * chains, LANES), jnp.float32), jnp.ones((4 * chains, LANES), jnp.float32))
        slot = lax.rem(l, 2)
        copy = pltpu.make_async_remote_copy(
            src_ref=mine_buf.at[slot],
            dst_ref=part_buf.at[slot],
            send_sem=send_sem.at[slot],
            recv_sem=recv_sem.at[slot],
            device_id=partner,
            device_id_type=MESH,
        )
        n_alone = len(ALONE)
        sums = [no_sums, no_sums]
        heights = (6 * chains, 6 * chains, 6 * chains, 8 * chains)
        totals = [[jnp.zeros((height, 256), jnp.float32) for height in heights] for _ in range(2)]
        resids = {}
        mine = None

        def logits_of(k, unit):
            return jnp.dot(weights, xt[k, unit * UNIT * FPAD : (unit + 1) * UNIT * FPAD, :], preferred_element_type=jnp.float32)

        def resids_of(u, which):
            h = jnp.tanh(u)
            pos_part = jnp.maximum(u, 0.0)
            fac = 1.0 + jnp.abs(h)
            pos_part = pos_part[: 4 * chains] + pos_part[4 * chains :]
            fac = fac[: 4 * chains] * fac[4 * chains :]
            ramp, prod = sums[which]
            sums[which] = (ramp + (pos_part[:, :LANES] + pos_part[:, LANES:]), prod * (fac[:, :LANES] * fac[:, LANES:]))
            return (1.0 + h).astype(jnp.bfloat16)

        def add_strip(which, strip, resid, cols):
            part = jnp.dot(resid, cols, preferred_element_type=jnp.float32)
            totals[which][strip] = totals[which][strip] + part

        def last_strips(which, ks):
            resid = jnp.concatenate([resids[k, 1][4 * chains :] for k in ks], axis=0)
            cols = jnp.concatenate([xs[k, :, 3 * 256 :] for k in ks], axis=1)
            if len(ks) == 1:
                part = jnp.dot(resid, cols, preferred_element_type=jnp.float32)
                zero_rows = jnp.zeros_like(part)
                part = jnp.concatenate([jnp.concatenate([part, zero_rows], axis=1), jnp.zeros((4 * chains, 256), jnp.float32)], axis=0)
                totals[which][3] = totals[which][3] + part
            else:
                add_strip(which, 3, resid, cols)

        def strips_of(k, stage):
            which = int(k >= n_alone)
            if stage == 0:
                add_strip(which, 0, resids[k, 0][: 6 * chains], xs[k, :, :256])
                mid = jnp.concatenate([resids[k, 0][4 * chains :], resids[k, 1][: 2 * chains]], axis=0)
                add_strip(which, 1, mid, xs[k, :, 256:512])
                return
            add_strip(which, 2, resids[k, 1][: 6 * chains], xs[k, :, 512:768])
            ends = k in (n_alone - 1, n_slots - 1)
            first = 0 if which == 0 else n_alone
            if (k - first) % 2:
                last_strips(which, [k - 1, k])
            elif ends:
                last_strips(which, [k])

        logits = {}
        units = 2 * n_slots
        for turn_no in range(units + GRAD_LAG):
            if turn_no < units:
                logits[turn_no] = logits_of(turn_no // 2, turn_no % 2)
            job = turn_no - MID_LAG
            if 0 <= job < units:
                resids[job // 2, job % 2] = resids_of(logits.pop(job), int(job // 2 >= n_alone))
            job = turn_no - GRAD_LAG
            if job >= 0:
                strips_of(job // 2, job % 2)
            if job == 2 * n_alone - 1 + SWAP_LAG:
                mine = gather_blocks(totals[0])
                mine_buf[slot] = mine
                copy.start()
        both = gather_blocks(totals[1])
        sums_alone, sums_both = sums

        kinetic = jnp.where(low, start_mom * start_mom * (0.5 / CORES), 0.0)
        hmat = jnp.where(lane == l - 2, jnp.sum(carried + kinetic, axis=1, keepdims=True), hmat)
        loss = fold(sums_alone) + (1.0 / CORES) * fold(sums_both)
        loss = loss + (n_chip * block_rows * BLOCKS // LANES) * LN2
        carried = loss + jnp.where(low, theta * theta * (0.5 / PRIOR_VAR / CORES), 0.0)

        copy.wait()
        grad = -0.5 * ((mine + part_buf[slot]) + both) - theta / PRIOR_VAR
        mom = mom + 0.5 * eps * grad
        return theta, mom, grad, carried, hmat

    zero = jnp.zeros((chains, LANES), jnp.float32)
    theta, mom, _, carried, hmat = lax.fori_loop(0, steps + 1, step_body, (theta0, mom0, zero, zero, zero))
    kinetic = jnp.where(low, mom * mom * (0.5 / CORES), 0.0)
    hmat = jnp.where(lane == steps - 1, jnp.sum(carried + kinetic, axis=1, keepdims=True), hmat)

    last = (steps + 1) % 2
    mine_buf[last] = hmat
    copy = pltpu.make_async_remote_copy(
        src_ref=mine_buf.at[last],
        dst_ref=part_buf.at[last],
        send_sem=send_sem.at[last],
        recv_sem=recv_sem.at[last],
        device_id=partner,
        device_id_type=MESH,
    )
    copy.start()
    copy.wait()

    rows = pl.ds(pl.multiple_of(chip * chains, chains), chains)
    gath_buf[1, rows, :] = theta + pltpu.roll(mom, LANES // 2, 1)
    gath_buf[2, rows, :] = hmat + part_buf[last]
    copies = []
    for off in range(1, n_chip):
        copies.append(
            pltpu.make_async_remote_copy(
                src_ref=gath_buf.at[pl.ds(1, 2), rows, :],
                dst_ref=gath_buf.at[pl.ds(1, 2), rows, :],
                send_sem=fin_send.at[off - 1],
                recv_sem=fin_recv.at[off - 1],
                device_id={"data": lax.rem(chip + off, n_chip) * CORES + core},
                device_id_type=MESH,
            )
        )
    for copy in copies:
        copy.start()
    for copy in copies:
        copy.wait()
    all_out[: LANES, :] = gath_buf[1].T
    all_out[LANES :, :] = gath_buf[2].T[:steps]


def solution(mesh):
    n_dev = mesh.shape["data"]
    n_chip = n_dev // CORES
    row_spec = P("data", None)
    chain_spec = P(None, "parts")

    def local_chains(feat_rows, labels, pos_init, mom_init, step_sizes):
        rows, feats = feat_rows.shape
        chains_all = pos_init.shape[1]
        steps = step_sizes.shape[0]
        chains = chains_all // n_chip
        block_rows = rows // BLOCKS

        vmem = pl.BlockSpec(memory_space=pltpu.VMEM)
        dma = pltpu.SemaphoreType.DMA
        slots = len(ALONE) + CORES * len(SHARED)
        ends = pl.pallas_call(
            functools.partial(chain_kernel, n_dev),
            out_shape=jax.ShapeDtypeStruct((LANES + steps, chains_all), jnp.float32),
            in_specs=[vmem] * 5,
            out_specs=vmem,
            scratch_shapes=[
                pltpu.VMEM((slots, block_rows, BLOCKS * FPAD), jnp.bfloat16),
                pltpu.VMEM((slots, BLOCKS * FPAD, block_rows), jnp.bfloat16),
                pltpu.VMEM((steps + 1, chains, LANES), jnp.float32),
                pltpu.VMEM((2, chains, LANES), jnp.float32),
                pltpu.VMEM((2, chains, LANES), jnp.float32),
                pltpu.VMEM((3, chains_all, LANES), jnp.float32),
                dma((2,)),
                dma((2,)),
                dma((n_chip - 1,)),
                dma((n_chip - 1,)),
                dma((40,)),
                dma((40,)),
                dma((2 * len(SHARED),)),
                dma((2 * len(SHARED),)),
            ],
            compiler_params=pltpu.CompilerParams(
                collective_id=0, has_side_effects=True, vmem_limit_bytes=60 * 1024 * 1024
            ),
        )(feat_rows.T, labels.reshape(rows // LANES, LANES), pos_init, mom_init, step_sizes)
        return ends[:feats], ends[LANES // 2 : LANES // 2 + feats], ends[LANES:]

    return jax.shard_map(local_chains, mesh=mesh, in_specs=(row_spec, P("data"), chain_spec, chain_spec, chain_spec), out_specs=(chain_spec, chain_spec, chain_spec), check_vma=False)
```

```python
import functools
import math

import jax
import jax.numpy as jnp
from jax import lax
from jax.experimental import pallas as pl
from jax.experimental.pallas import tpu as pltpu
from jax.sharding import PartitionSpec as P

PRIOR_VAR = 4.0
MESH = pl.DeviceIdType.MESH
CORES = 2
LANES = 128
FPAD = 56
BLOCKS = 16
UNIT = 4
MID_LAG, GRAD_LAG, SWAP_LAG = 5, 6, 5
LN2 = 0.6931471805599453
OFFSETS = [(dx, dy) for dy in (0, -1, 1, 2) for dx in (0, -1, 1, 2)]
SHARED = [(0, 0), (-1, 0), (1, 0)]
ALONE = [o for o in OFFSETS if o not in SHARED]


def chain_kernel(
    n_dev, rows_ref, label_ref, pos_ref, mom_ref, step_ref, all_out,
    xs, xt, eps_buf, part_buf, mine_buf, gath_buf,
    send_sem, recv_sem, fin_send, fin_recv, g_send, g_recv, d_send, d_recv,
):
    feats, chains_all = pos_ref.shape
    steps = step_ref.shape[0]
    n_chip = n_dev // CORES
    side = math.isqrt(n_chip)
    chains = chains_all // n_chip
    block_rows = xs.shape[1]
    width = BLOCKS * FPAD
    half_rows, quarter = width // 2, width // 4
    n_slots = len(ALONE) + CORES * len(SHARED)
    me = lax.axis_index("data")
    core = lax.rem(me, CORES)
    chip = me // CORES
    chip_x, chip_y = lax.rem(chip, side), chip // side
    lane = lax.broadcasted_iota(jnp.int32, (chains, LANES), 1)
    low = lane < feats
    partner = {"data": chip * CORES + 1 - core}

    def neighbour(axis, step):
        nx = lax.rem(chip_x + side + step, side) if axis == 0 else chip_x
        ny = lax.rem(chip_y + side + step, side) if axis == 1 else chip_y
        return {"data": (ny * side + nx) * CORES + core}

    barrier = pltpu.get_barrier_semaphore()
    for off in range(1, n_dev):
        pl.semaphore_signal(barrier, inc=1, device_id={"data": lax.rem(me + off, n_dev)}, device_id_type=MESH)

    def slot_of(offset):
        if offset in SHARED:
            return len(ALONE) + SHARED.index(offset) * CORES + core
        return ALONE.index(offset)

    sends = []

    def send(src, dst_slot, rows, sem, axis, step):
        copy = pltpu.make_async_remote_copy(
            src_ref=src,
            dst_ref=xt.at[dst_slot, rows, :],
            send_sem=g_send.at[len(sends)],
            recv_sem=g_recv.at[sem],
            device_id=neighbour(axis, step),
            device_id_type=MESH,
        )
        copy.start()
        sends.append(copy)

    def offset_of(half, first, second):
        return (first, second) if half == 0 else (second, first)

    def rows_of(half, part):
        if part is None:
            return pl.ds(half * half_rows, half_rows)
        return pl.ds(half * half_rows + part * quarter, quarter)

    kinds = [(1, None), (-1, None), (2, 0), (2, 1)]
    sem_ids = {}
    for half in range(2):
        for kind in kinds:
            sem_ids[half, kind[0], 0, kind[1]] = len(sem_ids)
            for first in (0, -1, 1, 2):
                sem_ids[half, first, kind[0], kind[1]] = len(sem_ids)

    def piece(half, first, second, part):
        return xt.at[slot_of(offset_of(half, first, second)), rows_of(half, part), :]

    def wrap(v):
        return 2 if v == -2 else v

    def pass_on(half, first, second, part, along, step, to_part=None):
        axis = along if half == 0 else 1 - along
        src_part = part if to_part is None else to_part
        src = piece(half, first, second, src_part)
        nf, ns = (wrap(first - step), second) if along == 0 else (first, wrap(second - step))
        key = (half, nf, ns, to_part)
        send(src, slot_of(offset_of(half, nf, ns)), rows_of(half, src_part), sem_ids[key], axis, step)

    def arrive(half, first, second, part):
        dst = piece(half, first, second, part)
        pltpu.make_async_copy(dst, dst, g_recv.at[sem_ids[half, first, second, part]]).wait()

    handed = []

    def hand_over(half, offset, src):
        index = SHARED.index(offset) * 2 + half
        copy = pltpu.make_async_remote_copy(
            src_ref=src,
            dst_ref=xt.at[slot_of(offset), rows_of(half, None), :],
            send_sem=d_send.at[index],
            recv_sem=d_recv.at[index],
            device_id=partner,
            device_id_type=MESH,
        )
        copy.start()
        handed.append(copy)

    seen = set()

    def turn(offset, half, slot):
        seen.add((offset, half))
        if (offset, 1 - half) not in seen:
            return

        def turn_part(i, _):
            rows = pl.ds(pl.multiple_of(i * LANES, LANES), LANES)
            xs[slot, :, rows] = xt[slot, rows, :].T
            return 0

        lax.fori_loop(0, width // LANES, turn_part, 0)

    own_slot = slot_of((0, 0))
    signs = (1 - 2 * label_ref[...]).astype(jnp.float32).astype(jnp.bfloat16)
    per_block = block_rows // LANES
    for j in range(BLOCKS * per_block):
        tile = rows_ref[:, j * LANES : (j + 1) * LANES] * signs[j : j + 1, :]
        tile = jnp.concatenate([tile, jnp.zeros((FPAD - feats, LANES), jnp.bfloat16)], axis=0)
        b, m = j // per_block, j % per_block
        xt[own_slot, b * FPAD : (b + 1) * FPAD, m * LANES : (m + 1) * LANES] = tile

    pl.semaphore_wait(barrier, n_dev - 1)
    for half in range(2):
        for step in (1, -1):
            pass_on(half, 0, 0, None, 0, step)
    for half in range(2):
        for step in (1, -1):
            pass_on(half, 0, 0, None, 1, step)
    for half in range(2):
        hand_over(half, (0, 0), piece(half, 0, 0, None))

    def own_rows(ref):
        rows = ref.shape[0]
        padded = jnp.concatenate([ref[...], jnp.zeros((LANES - rows, chains_all), jnp.float32)], axis=0)
        return padded.T

    def mine_of(ref, buf):
        buf[...] = own_rows(ref)
        return buf[pl.ds(pl.multiple_of(chip * chains, chains), chains), :]

    theta0 = mine_of(pos_ref, gath_buf.at[0])
    mom0 = mine_of(mom_ref, gath_buf.at[0])
    eps_rows = mine_of(step_ref, gath_buf.at[0])
    for l in range(steps):
        eps_buf[l + 1] = jnp.broadcast_to(eps_rows[:, l : l + 1], (chains, LANES))
    eps_buf[0] = jnp.zeros((chains, LANES), jnp.float32)
    for half in range(2):
        turn((0, 0), half, own_slot)

    def landed(half, first, second):
        offset = offset_of(half, first, second)
        if offset in SHARED:
            hand_over(half, offset, piece(half, first, second, None))

    fresh = []
    for half in range(2):
        for first in (-1, 1):
            arrive(half, first, 0, None)
            pass_on(half, first, 0, None, 0, -first, to_part=0 if first < 0 else 1)
            for step in (1, -1):
                pass_on(half, first, 0, None, 1, step)
            landed(half, first, 0)
            fresh.append((half, first, 0))

    def turn_fresh():
        for half, first, second in fresh:
            offset = offset_of(half, first, second)
            turn(offset, half, slot_of(offset))
        fresh.clear()

    turn_fresh()

    def second_ring(first):
        for half in range(2):
            for second in (-1, 1):
                arrive(half, first, second, None)
                pass_on(half, first, second, None, 1, -second, to_part=0 if second < 0 else 1)
                landed(half, first, second)
                fresh.append((half, first, second))

    second_ring(0)
    for half in range(2):
        for part in range(2):
            arrive(half, 2, 0, part)
        for step in (1, -1):
            pass_on(half, 2, 0, None, 1, step)
        fresh.append((half, 2, 0))
    turn_fresh()
    second_ring(-1)
    second_ring(1)
    turn_fresh()
    second_ring(2)
    for copy in handed:
        copy.wait_recv()
    for i, offset in enumerate(SHARED):
        for half in range(2):
            turn((offset, "partner"), half, len(ALONE) + i * CORES + 1 - core)
    for first in (0, -1, 1):
        for half in range(2):
            for part in range(2):
                arrive(half, first, 2, part)
            fresh.append((half, first, 2))
    turn_fresh()
    for half in range(2):
        for part in range(2):
            arrive(half, 2, 2, part)
        fresh.append((half, 2, 2))
    turn_fresh()
    for copy in sends:
        copy.wait_send()
    for copy in handed:
        copy.wait_send()

    def step_body(l, state):
        theta, mom, grad, carried, hmat = state
        eps = eps_buf[l]
        start_mom = mom
        mom = mom + 0.5 * eps * grad
        theta = theta + eps * mom

        half = 0.5 * theta
        none = jnp.zeros_like(half)
        rows_w = []
        for b in range(UNIT):
            col, start = b * FPAD // LANES, b * FPAD % LANES
            moved = pltpu.roll(half, start, 1) if start else half
            cols = [none] * (-(-UNIT * FPAD // LANES))
            if start + FPAD <= LANES:
                cols[col] = moved
            else:
                cols[col] = jnp.where(lane >= start, moved, 0.0)
                cols[col + 1] = jnp.where(lane >= start, 0.0, moved)
            rows_w.append(jnp.concatenate(cols, axis=1))
        weights = jnp.concatenate(rows_w, axis=0).astype(jnp.bfloat16)[:, : UNIT * FPAD]

        first_block = (0, 4, 8, 12)

        def gather_blocks(strips):
            result = None
            for b in range(BLOCKS):
                col, start = b * FPAD // LANES, b * FPAD % LANES

                def at(c):
                    strip = c // 2
                    row = (b - first_block[strip]) * chains
                    if strip < 3:
                        return strips[strip][row : row + chains, (c % 2) * LANES : (c % 2 + 1) * LANES]
                    other = row + 4 * chains
                    return strips[3][row : row + chains, :LANES] + strips[3][other : other + chains, LANES:]

                part = at(col)
                if start + feats > LANES:
                    part = jnp.where(lane >= start, part, at(col + 1))
                part = pltpu.roll(part, LANES - start, 1) if start else part
                result = part if result is None else result + part
            return jnp.where(low, result, 0.0)

        def fold(sums):
            loss = 2.0 * sums[0] - jnp.log(sums[1])
            return loss[:chains] + loss[chains : 2 * chains] + loss[2 * chains : 3 * chains] + loss[3 * chains :]

        no_sums = (jnp.zeros((4 * chains, LANES), jnp.float32), jnp.ones((4 * chains, LANES), jnp.float32))
        slot = lax.rem(l, 2)
        copy = pltpu.make_async_remote_copy(
            src_ref=mine_buf.at[slot],
            dst_ref=part_buf.at[slot],
            send_sem=send_sem.at[slot],
            recv_sem=recv_sem.at[slot],
            device_id=partner,
            device_id_type=MESH,
        )
        n_alone = len(ALONE)
        sums = [no_sums, no_sums]
        heights = (6 * chains, 6 * chains, 6 * chains, 8 * chains)
        totals = [[jnp.zeros((height, 256), jnp.float32) for height in heights] for _ in range(2)]
        resids = {}
        mine = None

        def logits_of(k, unit):
            return jnp.dot(weights, xt[k, unit * UNIT * FPAD : (unit + 1) * UNIT * FPAD, :], preferred_element_type=jnp.float32)

        def resids_of(u, which):
            h = jnp.tanh(u)
            pos_part = jnp.maximum(u, 0.0)
            fac = 1.0 + jnp.abs(h)
            ramp, prod = sums[which]
            sums[which] = (ramp + (pos_part[:, :LANES] + pos_part[:, LANES:]), prod * (fac[:, :LANES] * fac[:, LANES:]))
            return (1.0 + h).astype(jnp.bfloat16)

        def add_strip(which, strip, resid, cols):
            part = jnp.dot(resid, cols, preferred_element_type=jnp.float32)
            totals[which][strip] = totals[which][strip] + part

        def last_strips(which, ks):
            resid = jnp.concatenate([resids[k, 3] for k in ks], axis=0)
            cols = jnp.concatenate([xs[k, :, 3 * 256 :] for k in ks], axis=1)
            if len(ks) == 1:
                part = jnp.dot(resid, cols, preferred_element_type=jnp.float32)
                zero_rows = jnp.zeros_like(part)
                part = jnp.concatenate([jnp.concatenate([part, zero_rows], axis=1), jnp.zeros((4 * chains, 256), jnp.float32)], axis=0)
                totals[which][3] = totals[which][3] + part
            else:
                add_strip(which, 3, resid, cols)

        def strips_of(k, unit):
            which = int(k >= n_alone)
            if unit == 0:
                return
            resid = jnp.concatenate([resids[k, unit - 1], resids[k, unit][: 2 * chains]], axis=0)
            add_strip(which, unit - 1, resid, xs[k, :, (unit - 1) * 256 : unit * 256])
            if unit < 3:
                return
            ends = k in (n_alone - 1, n_slots - 1)
            first = 0 if which == 0 else n_alone
            if (k - first) % 2:
                last_strips(which, [k - 1, k])
            elif ends:
                last_strips(which, [k])

        logits = {}
        per = BLOCKS // UNIT
        units = per * n_slots
        for turn_no in range(units + GRAD_LAG):
            if turn_no < units:
                logits[turn_no] = logits_of(turn_no // per, turn_no % per)
            job = turn_no - MID_LAG
            if 0 <= job < units:
                resids[job // per, job % per] = resids_of(logits.pop(job), int(job // per >= n_alone))
            job = turn_no - GRAD_LAG
            if job >= 0:
                strips_of(job // per, job % per)
            if job == per * n_alone - 1 + SWAP_LAG:
                mine = gather_blocks(totals[0])
                mine_buf[slot] = mine
                copy.start()
        both = gather_blocks(totals[1])
        sums_alone, sums_both = sums

        kinetic = jnp.where(low, start_mom * start_mom * (0.5 / CORES), 0.0)
        hmat = jnp.where(lane == l - 2, jnp.sum(carried + kinetic, axis=1, keepdims=True), hmat)
        loss = fold(sums_alone) + (1.0 / CORES) * fold(sums_both)
        loss = loss + (n_chip * block_rows * BLOCKS // LANES) * LN2
        carried = loss + jnp.where(low, theta * theta * (0.5 / PRIOR_VAR / CORES), 0.0)

        copy.wait()
        grad = -0.5 * ((mine + part_buf[slot]) + both) - theta / PRIOR_VAR
        mom = mom + 0.5 * eps * grad
        return theta, mom, grad, carried, hmat

    zero = jnp.zeros((chains, LANES), jnp.float32)
    theta, mom, _, carried, hmat = lax.fori_loop(0, steps + 1, step_body, (theta0, mom0, zero, zero, zero))
    kinetic = jnp.where(low, mom * mom * (0.5 / CORES), 0.0)
    hmat = jnp.where(lane == steps - 1, jnp.sum(carried + kinetic, axis=1, keepdims=True), hmat)

    last = (steps + 1) % 2
    mine_buf[last] = hmat
    copy = pltpu.make_async_remote_copy(
        src_ref=mine_buf.at[last],
        dst_ref=part_buf.at[last],
        send_sem=send_sem.at[last],
        recv_sem=recv_sem.at[last],
        device_id=partner,
        device_id_type=MESH,
    )
    copy.start()
    copy.wait()

    rows = pl.ds(pl.multiple_of(chip * chains, chains), chains)
    gath_buf[1, rows, :] = theta + pltpu.roll(mom, LANES // 2, 1)
    gath_buf[2, rows, :] = hmat + part_buf[last]
    copies = []
    for off in range(1, n_chip):
        copies.append(
            pltpu.make_async_remote_copy(
                src_ref=gath_buf.at[pl.ds(1, 2), rows, :],
                dst_ref=gath_buf.at[pl.ds(1, 2), rows, :],
                send_sem=fin_send.at[off - 1],
                recv_sem=fin_recv.at[off - 1],
                device_id={"data": lax.rem(chip + off, n_chip) * CORES + core},
                device_id_type=MESH,
            )
        )
    for copy in copies:
        copy.start()
    for copy in copies:
        copy.wait()
    all_out[: LANES, :] = gath_buf[1].T
    all_out[LANES :, :] = gath_buf[2].T[:steps]


def solution(mesh):
    n_dev = mesh.shape["data"]
    n_chip = n_dev // CORES
    row_spec = P("data", None)
    chain_spec = P(None, "parts")

    def local_chains(feat_rows, labels, pos_init, mom_init, step_sizes):
        rows, feats = feat_rows.shape
        chains_all = pos_init.shape[1]
        steps = step_sizes.shape[0]
        chains = chains_all // n_chip
        block_rows = rows // BLOCKS

        vmem = pl.BlockSpec(memory_space=pltpu.VMEM)
        dma = pltpu.SemaphoreType.DMA
        slots = len(ALONE) + CORES * len(SHARED)
        ends = pl.pallas_call(
            functools.partial(chain_kernel, n_dev),
            out_shape=jax.ShapeDtypeStruct((LANES + steps, chains_all), jnp.float32),
            in_specs=[vmem] * 5,
            out_specs=vmem,
            scratch_shapes=[
                pltpu.VMEM((slots, block_rows, BLOCKS * FPAD), jnp.bfloat16),
                pltpu.VMEM((slots, BLOCKS * FPAD, block_rows), jnp.bfloat16),
                pltpu.VMEM((steps + 1, chains, LANES), jnp.float32),
                pltpu.VMEM((2, chains, LANES), jnp.float32),
                pltpu.VMEM((2, chains, LANES), jnp.float32),
                pltpu.VMEM((3, chains_all, LANES), jnp.float32),
                dma((2,)),
                dma((2,)),
                dma((n_chip - 1,)),
                dma((n_chip - 1,)),
                dma((40,)),
                dma((40,)),
                dma((2 * len(SHARED),)),
                dma((2 * len(SHARED),)),
            ],
            compiler_params=pltpu.CompilerParams(
                collective_id=0, has_side_effects=True, vmem_limit_bytes=60 * 1024 * 1024
            ),
        )(feat_rows.T, labels.reshape(rows // LANES, LANES), pos_init, mom_init, step_sizes)
        return ends[:feats], ends[LANES // 2 : LANES // 2 + feats], ends[LANES:]

    return jax.shard_map(local_chains, mesh=mesh, in_specs=(row_spec, P("data"), chain_spec, chain_spec, chain_spec), out_specs=(chain_spec, chain_spec, chain_spec), check_vma=False)
```

```python
import functools
import math

import jax
import jax.numpy as jnp
from jax import lax
from jax.experimental import pallas as pl
from jax.experimental.pallas import tpu as pltpu
from jax.sharding import PartitionSpec as P

PRIOR_VAR = 4.0
MESH = pl.DeviceIdType.MESH
CORES = 2
LANES = 128
FPAD = 56
BLOCKS = 16
UNIT = 4
MID_LAG, GRAD_LAG, SWAP_LAG = 5, 6, 5
LN2 = 0.6931471805599453
OFFSETS = [(dx, dy) for dy in (0, -1, 1, 2) for dx in (0, -1, 1, 2)]
SHARED = [(0, 0), (-1, 0), (1, 0)]
ALONE = [o for o in OFFSETS if o not in SHARED]


def chain_kernel(
    n_dev, rows_ref, label_ref, pos_ref, mom_ref, step_ref, all_out,
    xs, xt, eps_buf, part_buf, mine_buf, gath_buf,
    send_sem, recv_sem, fin_send, fin_recv, g_send, g_recv, d_send, d_recv,
):
    feats, chains_all = pos_ref.shape
    steps = step_ref.shape[0]
    n_chip = n_dev // CORES
    side = math.isqrt(n_chip)
    chains = chains_all // n_chip
    block_rows = xs.shape[1]
    width = BLOCKS * FPAD
    half_rows, quarter = width // 2, width // 4
    n_slots = len(ALONE) + CORES * len(SHARED)
    me = lax.axis_index("data")
    core = lax.rem(me, CORES)
    chip = me // CORES
    chip_x, chip_y = lax.rem(chip, side), chip // side
    lane = lax.broadcasted_iota(jnp.int32, (chains, LANES), 1)
    low = lane < feats
    partner = {"data": chip * CORES + 1 - core}

    def neighbour(axis, step):
        nx = lax.rem(chip_x + side + step, side) if axis == 0 else chip_x
        ny = lax.rem(chip_y + side + step, side) if axis == 1 else chip_y
        return {"data": (ny * side + nx) * CORES + core}

    barrier = pltpu.get_barrier_semaphore()
    for off in range(1, n_dev):
        pl.semaphore_signal(barrier, inc=1, device_id={"data": lax.rem(me + off, n_dev)}, device_id_type=MESH)

    def slot_of(offset):
        if offset in SHARED:
            return len(ALONE) + SHARED.index(offset) * CORES + core
        return ALONE.index(offset)

    sends = []

    def send(src, dst_slot, rows, sem, axis, step):
        copy = pltpu.make_async_remote_copy(
            src_ref=src,
            dst_ref=xt.at[dst_slot, rows, :],
            send_sem=g_send.at[len(sends)],
            recv_sem=g_recv.at[sem],
            device_id=neighbour(axis, step),
            device_id_type=MESH,
        )
        copy.start()
        sends.append(copy)

    def offset_of(half, first, second):
        return (first, second) if half == 0 else (second, first)

    def rows_of(half, part):
        if part is None:
            return pl.ds(half * half_rows, half_rows)
        return pl.ds(half * half_rows + part * quarter, quarter)

    kinds = [(1, None), (-1, None), (2, 0), (2, 1)]
    sem_ids = {}
    for half in range(2):
        for kind in kinds:
            sem_ids[half, kind[0], 0, kind[1]] = len(sem_ids)
            for first in (0, -1, 1, 2):
                sem_ids[half, first, kind[0], kind[1]] = len(sem_ids)

    def piece(half, first, second, part):
        return xt.at[slot_of(offset_of(half, first, second)), rows_of(half, part), :]

    def wrap(v):
        return 2 if v == -2 else v

    def pass_on(half, first, second, part, along, step, to_part=None):
        axis = along if half == 0 else 1 - along
        src_part = part if to_part is None else to_part
        src = piece(half, first, second, src_part)
        nf, ns = (wrap(first - step), second) if along == 0 else (first, wrap(second - step))
        key = (half, nf, ns, to_part)
        send(src, slot_of(offset_of(half, nf, ns)), rows_of(half, src_part), sem_ids[key], axis, step)

    def arrive(half, first, second, part):
        dst = piece(half, first, second, part)
        pltpu.make_async_copy(dst, dst, g_recv.at[sem_ids[half, first, second, part]]).wait()

    handed = []

    def hand_over(half, offset, src):
        index = SHARED.index(offset) * 2 + half
        copy = pltpu.make_async_remote_copy(
            src_ref=src,
            dst_ref=xt.at[slot_of(offset), rows_of(half, None), :],
            send_sem=d_send.at[index],
            recv_sem=d_recv.at[index],
            device_id=partner,
            device_id_type=MESH,
        )
        copy.start()
        handed.append(copy)

    seen = set()

    def turn(offset, half, slot):
        seen.add((offset, half))
        if (offset, 1 - half) not in seen:
            return

        def turn_part(i, _):
            rows = pl.ds(pl.multiple_of(i * LANES, LANES), LANES)
            xs[slot, :, rows] = xt[slot, rows, :].T
            return 0

        lax.fori_loop(0, width // LANES, turn_part, 0)

    own_slot = slot_of((0, 0))
    signs = (1 - 2 * label_ref[...]).astype(jnp.float32).astype(jnp.bfloat16)
    per_block = block_rows // LANES
    for j in range(BLOCKS * per_block):
        tile = rows_ref[:, j * LANES : (j + 1) * LANES] * signs[j : j + 1, :]
        tile = jnp.concatenate([tile, jnp.zeros((FPAD - feats, LANES), jnp.bfloat16)], axis=0)
        b, m = j // per_block, j % per_block
        xt[own_slot, b * FPAD : (b + 1) * FPAD, m * LANES : (m + 1) * LANES] = tile

    pl.semaphore_wait(barrier, n_dev - 1)
    for half in range(2):
        for step in (1, -1):
            pass_on(half, 0, 0, None, 0, step)
    for half in range(2):
        for step in (1, -1):
            pass_on(half, 0, 0, None, 1, step)
    for half in range(2):
        hand_over(half, (0, 0), piece(half, 0, 0, None))

    def own_rows(ref):
        rows = ref.shape[0]
        padded = jnp.concatenate([ref[...], jnp.zeros((LANES - rows, chains_all), jnp.float32)], axis=0)
        return padded.T

    def mine_of(ref, buf):
        buf[...] = own_rows(ref)
        return buf[pl.ds(pl.multiple_of(chip * chains, chains), chains), :]

    theta0 = mine_of(pos_ref, gath_buf.at[3])
    mom0 = mine_of(mom_ref, gath_buf.at[3])
    eps_rows = mine_of(step_ref, gath_buf.at[3])
    for l in range(steps):
        eps_buf[l + 1] = jnp.broadcast_to(eps_rows[:, l : l + 1], (chains, LANES))
    eps_buf[0] = jnp.zeros((chains, LANES), jnp.float32)
    for half in range(2):
        turn((0, 0), half, own_slot)

    def landed(half, first, second):
        offset = offset_of(half, first, second)
        if offset in SHARED:
            hand_over(half, offset, piece(half, first, second, None))

    fresh = []
    for half in range(2):
        for first in (-1, 1):
            arrive(half, first, 0, None)
            pass_on(half, first, 0, None, 0, -first, to_part=0 if first < 0 else 1)
            for step in (1, -1):
                pass_on(half, first, 0, None, 1, step)
            landed(half, first, 0)
            fresh.append((half, first, 0))

    def turn_fresh():
        for half, first, second in fresh:
            offset = offset_of(half, first, second)
            turn(offset, half, slot_of(offset))
        fresh.clear()

    turn_fresh()

    def second_ring(first):
        for half in range(2):
            for second in (-1, 1):
                arrive(half, first, second, None)
                pass_on(half, first, second, None, 1, -second, to_part=0 if second < 0 else 1)
                landed(half, first, second)
                fresh.append((half, first, second))

    second_ring(0)
    for half in range(2):
        for part in range(2):
            arrive(half, 2, 0, part)
        for step in (1, -1):
            pass_on(half, 2, 0, None, 1, step)
        fresh.append((half, 2, 0))
    turn_fresh()
    second_ring(-1)
    second_ring(1)
    turn_fresh()
    second_ring(2)
    for copy in handed:
        copy.wait_recv()
    for i, offset in enumerate(SHARED):
        for half in range(2):
            turn((offset, "partner"), half, len(ALONE) + i * CORES + 1 - core)
    for first in (0, -1, 1):
        for half in range(2):
            for part in range(2):
                arrive(half, first, 2, part)
            fresh.append((half, first, 2))
    turn_fresh()
    for half in range(2):
        for part in range(2):
            arrive(half, 2, 2, part)
        fresh.append((half, 2, 2))
    turn_fresh()
    for copy in sends:
        copy.wait_send()
    for copy in handed:
        copy.wait_send()

    def step_body(l, state):
        theta, mom, grad, carried, hmat = state
        eps = eps_buf[l]
        start_mom = mom
        mom = mom + 0.5 * eps * grad
        theta = theta + eps * mom

        half = 0.5 * theta
        none = jnp.zeros_like(half)
        rows_w = []
        for b in range(UNIT):
            col, start = b * FPAD // LANES, b * FPAD % LANES
            moved = pltpu.roll(half, start, 1) if start else half
            cols = [none] * (-(-UNIT * FPAD // LANES))
            if start + FPAD <= LANES:
                cols[col] = moved
            else:
                cols[col] = jnp.where(lane >= start, moved, 0.0)
                cols[col + 1] = jnp.where(lane >= start, 0.0, moved)
            rows_w.append(jnp.concatenate(cols, axis=1))
        weights = jnp.concatenate(rows_w, axis=0).astype(jnp.bfloat16)[:, : UNIT * FPAD]

        first_block = (0, 4, 8, 12)

        def gather_blocks(strips):
            result = None
            for b in range(BLOCKS):
                col, start = b * FPAD // LANES, b * FPAD % LANES

                def at(c):
                    strip = c // 2
                    row = (b - first_block[strip]) * chains
                    if strip < 3:
                        return strips[strip][row : row + chains, (c % 2) * LANES : (c % 2 + 1) * LANES]
                    other = row + 4 * chains
                    return strips[3][row : row + chains, :LANES] + strips[3][other : other + chains, LANES:]

                part = at(col)
                if start + feats > LANES:
                    part = jnp.where(lane >= start, part, at(col + 1))
                part = pltpu.roll(part, LANES - start, 1) if start else part
                result = part if result is None else result + part
            return jnp.where(low, result, 0.0)

        def fold(sums):
            loss = 2.0 * sums[0] - jnp.log(sums[1])
            return loss[:chains] + loss[chains : 2 * chains] + loss[2 * chains : 3 * chains] + loss[3 * chains :]

        no_sums = (jnp.zeros((4 * chains, LANES), jnp.float32), jnp.ones((4 * chains, LANES), jnp.float32))
        slot = lax.rem(l, 2)
        copy = pltpu.make_async_remote_copy(
            src_ref=mine_buf.at[slot],
            dst_ref=part_buf.at[slot],
            send_sem=send_sem.at[slot],
            recv_sem=recv_sem.at[slot],
            device_id=partner,
            device_id_type=MESH,
        )
        n_alone = len(ALONE)
        sums = [no_sums, no_sums]
        heights = (6 * chains, 6 * chains, 6 * chains, 8 * chains)
        totals = [[jnp.zeros((height, 256), jnp.float32) for height in heights] for _ in range(2)]
        resids = {}
        mine = None

        def logits_of(k, unit):
            return jnp.dot(weights, xt[k, unit * UNIT * FPAD : (unit + 1) * UNIT * FPAD, :], preferred_element_type=jnp.float32)

        def resids_of(u, which):
            h = jnp.tanh(u)
            pos_part = jnp.maximum(u, 0.0)
            fac = 1.0 + jnp.abs(h)
            ramp, prod = sums[which]
            sums[which] = (ramp + (pos_part[:, :LANES] + pos_part[:, LANES:]), prod * (fac[:, :LANES] * fac[:, LANES:]))
            return (1.0 + h).astype(jnp.bfloat16)

        def add_strip(which, strip, resid, cols):
            part = jnp.dot(resid, cols, preferred_element_type=jnp.float32)
            totals[which][strip] = totals[which][strip] + part

        def last_strips(which, ks):
            resid = jnp.concatenate([resids[k, 3] for k in ks], axis=0)
            cols = jnp.concatenate([xs[k, :, 3 * 256 :] for k in ks], axis=1)
            if len(ks) == 1:
                part = jnp.dot(resid, cols, preferred_element_type=jnp.float32)
                zero_rows = jnp.zeros_like(part)
                part = jnp.concatenate([jnp.concatenate([part, zero_rows], axis=1), jnp.zeros((4 * chains, 256), jnp.float32)], axis=0)
                totals[which][3] = totals[which][3] + part
            else:
                add_strip(which, 3, resid, cols)

        def strips_of(k, unit):
            which = int(k >= n_alone)
            if unit == 0:
                return
            resid = jnp.concatenate([resids[k, unit - 1], resids[k, unit][: 2 * chains]], axis=0)
            add_strip(which, unit - 1, resid, xs[k, :, (unit - 1) * 256 : unit * 256])
            if unit < 3:
                return
            ends = k in (n_alone - 1, n_slots - 1)
            first = 0 if which == 0 else n_alone
            if (k - first) % 2:
                last_strips(which, [k - 1, k])
            elif ends:
                last_strips(which, [k])

        logits = {}
        per = BLOCKS // UNIT
        units = per * n_slots
        for turn_no in range(units + GRAD_LAG):
            if turn_no < units:
                logits[turn_no] = logits_of(turn_no // per, turn_no % per)
            job = turn_no - MID_LAG
            if 0 <= job < units:
                resids[job // per, job % per] = resids_of(logits.pop(job), int(job // per >= n_alone))
            job = turn_no - GRAD_LAG
            if job >= 0:
                strips_of(job // per, job % per)
            if job == per * n_alone - 1 + SWAP_LAG:
                mine = gather_blocks(totals[0])
                mine_buf[slot] = mine
                copy.start()
        both = gather_blocks(totals[1])
        sums_alone, sums_both = sums

        kinetic = jnp.where(low, start_mom * start_mom * (0.5 / CORES), 0.0)
        hmat = jnp.where(lane == l - 2, jnp.sum(carried + kinetic, axis=1, keepdims=True), hmat)
        loss = fold(sums_alone) + (1.0 / CORES) * fold(sums_both)
        loss = loss + (n_chip * block_rows * BLOCKS // LANES) * LN2
        carried = loss + jnp.where(low, theta * theta * (0.5 / PRIOR_VAR / CORES), 0.0)

        copy.wait()
        grad = -0.5 * ((mine + part_buf[slot]) + both) - theta / PRIOR_VAR
        mom = mom + 0.5 * eps * grad
        return theta, mom, grad, carried, hmat

    zero = jnp.zeros((chains, LANES), jnp.float32)
    theta, mom, _, carried, hmat = lax.fori_loop(0, steps + 1, step_body, (theta0, mom0, zero, zero, zero))
    kinetic = jnp.where(low, mom * mom * (0.5 / CORES), 0.0)
    hmat = jnp.where(lane == steps - 1, jnp.sum(carried + kinetic, axis=1, keepdims=True), hmat)

    rows = pl.ds(pl.multiple_of(chip * chains, chains), chains)
    gath_buf[0, rows, :] = theta + pltpu.roll(mom, LANES // 2, 1)
    gath_buf[1 + core, rows, :] = hmat
    copies = []

    def spread(plane, device):
        part = gath_buf.at[plane, rows, :]
        sems = (fin_send.at[len(copies)], fin_recv.at[len(copies)])
        copies.append(pltpu.make_async_remote_copy(part, part, *sems, device_id={"data": device}, device_id_type=MESH))

    for off in range(1, n_chip):
        other = lax.rem(chip + off, n_chip) * CORES
        spread(0, other + core)
        spread(1 + core, other + core)
        spread(1 + core, other + 1 - core)
    spread(1 + core, chip * CORES + 1 - core)
    for copy in copies:
        copy.start()
    for copy in copies:
        copy.wait_send()
    arrived = 0
    for off in range(1, n_chip):
        origin = pl.ds(pl.multiple_of(lax.rem(chip + n_chip - off, n_chip) * chains, chains), chains)
        for plane in (0, 1 + core, 2 - core):
            part = gath_buf.at[plane, origin, :]
            pltpu.make_async_copy(part, part, fin_recv.at[arrived]).wait()
            arrived += 1
    part = gath_buf.at[2 - core, rows, :]
    pltpu.make_async_copy(part, part, fin_recv.at[arrived]).wait()
    all_out[: LANES, :] = gath_buf[0].T
    all_out[LANES :, :] = (gath_buf[1] + gath_buf[2]).T[:steps]


def solution(mesh):
    n_dev = mesh.shape["data"]
    n_chip = n_dev // CORES
    row_spec = P("data", None)
    chain_spec = P(None, "parts")

    def local_chains(feat_rows, labels, pos_init, mom_init, step_sizes):
        rows, feats = feat_rows.shape
        chains_all = pos_init.shape[1]
        steps = step_sizes.shape[0]
        chains = chains_all // n_chip
        block_rows = rows // BLOCKS

        vmem = pl.BlockSpec(memory_space=pltpu.VMEM)
        dma = pltpu.SemaphoreType.DMA
        slots = len(ALONE) + CORES * len(SHARED)
        ends = pl.pallas_call(
            functools.partial(chain_kernel, n_dev),
            out_shape=jax.ShapeDtypeStruct((LANES + steps, chains_all), jnp.float32),
            in_specs=[vmem] * 5,
            out_specs=vmem,
            scratch_shapes=[
                pltpu.VMEM((slots, block_rows, BLOCKS * FPAD), jnp.bfloat16),
                pltpu.VMEM((slots, BLOCKS * FPAD, block_rows), jnp.bfloat16),
                pltpu.VMEM((steps + 1, chains, LANES), jnp.float32),
                pltpu.VMEM((2, chains, LANES), jnp.float32),
                pltpu.VMEM((2, chains, LANES), jnp.float32),
                pltpu.VMEM((4, chains_all, LANES), jnp.float32),
                dma((2,)),
                dma((2,)),
                dma((3 * n_chip - 2,)),
                dma((3 * n_chip - 2,)),
                dma((40,)),
                dma((40,)),
                dma((2 * len(SHARED),)),
                dma((2 * len(SHARED),)),
            ],
            compiler_params=pltpu.CompilerParams(
                collective_id=0, has_side_effects=True, vmem_limit_bytes=60 * 1024 * 1024
            ),
        )(feat_rows.T, labels.reshape(rows // LANES, LANES), pos_init, mom_init, step_sizes)
        return ends[:feats], ends[LANES // 2 : LANES // 2 + feats], ends[LANES:]

    return jax.shard_map(local_chains, mesh=mesh, in_specs=(row_spec, P("data"), chain_spec, chain_spec, chain_spec), out_specs=(chain_spec, chain_spec, chain_spec), check_vma=False)
```
